32 devices in a mesh: gx: 8 (over y, x, core), gy: 4 (over z).
Axes of the slice: x: 2, y: 2, z: 4, core: 2. Of those that a mesh axis runs over, the one named last changes fastest.
Arguments:
- disc_pos: float32 [2, 32, 128, 128], P(None, 'gy', 'gx'), may hold values from 0 to 1
- disc_vel: float32 [2, 32, 128, 128], P(None, 'gy', 'gx'), may hold values from -3 to 3
- radius: float32 [32, 128, 128], P('gy', 'gx'), may hold values from 0.04 to 0.08
- bond_list: int32 [4, 32, 128, 128], P(None, 'gy', 'gx'), may hold values from 0 to 127
- contact_mask: int32 [8, 32, 128], P(None, 'gy', 'gx'), may hold values 0 or 1
- remap_block: int32 [32, 32, 8], P(('gx', 'gy')), may hold values from -1 to 127, as said below
- ocean_state: float32 [4, 48, 128, 1024], P(None, None, 'gy', 'gx'), may hold values from -6 to 6
- mix_coef: float32 [48, 128, 1024], P(None, 'gy', 'gx'), may hold values from 0.02 to 0.2
- remap_cell: int32 [32, 32, 8], P(('gx', 'gy')), may hold values from 0 to 4095
- fold_perm: int32 [1024], P('gx'), may hold values from 0 to 1023, as said below
Outputs:
- pos_next: float32 [2, 32, 128, 128], P(None, 'gy', 'gx')
- vel_next: float32 [2, 32, 128, 128], P(None, 'gy', 'gx')
- ocean_next: float32 [4, 48, 128, 1024], P(None, None, 'gy', 'gx')
The draws below stay inside these ranges and needn't reach their ends.
Inputs may be any that keep to these rules, and one draw needn't show every extreme that they name: `remap_block`: for each ice tile, every one of its 128 local blocks stands in exactly one slot and the other slots hold -1; in every draw some ocean tile gets all 8 of its slots filled by every ice tile. `fold_perm`: A permutation of the 1024 columns.
All inputs are finite; a program needn't handle non-finite values. No bound on the sum of `contact_mask` on one device may be relied on, other than what follows from the above.
Results may differ from the reference program's by a relative error of at most 0.0003.
Values sent between devices are 32-bit elements; how exact they have to be, the bound alone decides.
No kernel may reach another device: no remote copies, remote signals or barrier semaphores. Data moves between devices by JAX's collectives and lax.ppermute only.
A program may use at most 128 MiB of HBM per device.

```python
import math
import jax
import jax.numpy as jnp
from jax import lax

DISCS = 128
BONDS = 4
SUB = 3
KL = 48
BGX = 16
BGY = 8
OX = 128
OY = 32
NBX = 128
NBY = 32
TILES = 32
CAP = 8
NXO = 1024
NYO = 128
OCELLS = 4096
N_GX = 8
N_GY = 4


def draw_remap_block(key, part):
    blocks = BGX * BGY
    slots = TILES * CAP
    full_tile = jax.random.randint(jax.random.fold_in(key, 11), (), 0, TILES)
    slot_ids = jnp.arange(slots, dtype=jnp.int32)

    def one_source(source):
        scores = jax.random.permutation(jax.random.fold_in(key, 1000 + source), slots).astype(jnp.int32)
        scores = jnp.where(slot_ids // CAP == full_tile, slot_ids % CAP - CAP, scores)
        order = jnp.argsort(scores, stable=True)
        table = jnp.full((slots,), -1, jnp.int32).at[order[:blocks]].set(jnp.arange(blocks, dtype=jnp.int32))
        return table.reshape(TILES, CAP)
    return jax.vmap(one_source)(jnp.arange(TILES, dtype=jnp.int32))


def draw_fold_perm(key, part):
    return jax.random.permutation(jax.random.fold_in(key, 23), NXO).astype(jnp.int32)


def set_ends(values, own_key, low, top_value):
    shape = values.shape
    spot = [jax.random.randint(jax.random.fold_in(own_key, axis), (), 0, shape[axis]) for axis in range(len(shape))]
    values = values.at[tuple(spot)].set(low)
    longest = shape.index(max(shape))
    spot[longest] = (spot[longest] + 1) % shape[longest]
    return values.at[tuple(spot)].set(top_value)


def block_levels(own_key, dims, shards, smallest, high):
    loudness = 1.0
    for dim, shards_of in shards:
        heights = jax.random.uniform(jax.random.fold_in(jax.random.fold_in(own_key, 6), dim), (shards_of,), jnp.float32, smallest / len(shards), high / len(shards))
        loudness = loudness * jnp.repeat(jnp.exp(heights), dims[dim] // shards_of).reshape((-1,) + (1,) * (len(dims) - 1 - dim))
    return loudness


def normal_values(own_key, extent, scale, most, pieces=(), kind=jnp.bfloat16):
    values = jax.random.normal(own_key, extent, jnp.float32) * scale
    if len(pieces) > 0:
        values = block_levels(own_key, extent, pieces, -0.22, 0.18) * values
    return jnp.clip(values, min=-most, max=most).astype(kind)


def setup_inputs(seed: int = 0) -> dict:
    key_list = jax.random.split(jax.random.key(seed), 11)
    disc_pos = jnp.clip(1.0 * jax.random.uniform(key_list[0], (2, NBY, NBX, DISCS), jnp.float32) ** block_levels(key_list[0], (2, NBY, NBX, DISCS), ((1, 4), (2, 8)), -0.2, 0.2), 0.0, 1.0)
    disc_vel = normal_values(key_list[1], (2, NBY, NBX, DISCS), 0.5, 3.0, ((1, 4), (2, 8)), jnp.float32)
    radius = jnp.clip(0.04 + 0.04 * jax.random.uniform(key_list[2], (NBY, NBX, DISCS), jnp.float32) ** block_levels(key_list[2], (NBY, NBX, DISCS), ((0, 4), (1, 8)), -0.2, 0.2), 0.04, 0.08)
    bond_list = set_ends(jax.random.randint(key_list[3], (BONDS, NBY, NBX, DISCS), 0, DISCS), jax.random.fold_in(key_list[3], 1), 0, DISCS - 1).astype(jnp.int32)
    contact_mask = set_ends((jax.random.randint(key_list[4], (8, NBY, NBX), 0, 2) < 1).astype(jnp.int32), jax.random.fold_in(key_list[4], 1), 0, 1)
    remap_block = draw_remap_block(jax.random.fold_in(key_list[10], 71), 0)
    ocean_state = normal_values(key_list[6], (4, KL, NYO, NXO), 1.0, 6.0, ((2, 4), (3, 8)), jnp.float32)
    mix_coef = jnp.clip(jnp.exp(math.log(0.2) - 2.3025851 * jax.random.uniform(key_list[7], (KL, NYO, NXO), jnp.float32) ** block_levels(key_list[7], (KL, NYO, NXO), ((1, 4), (2, 8)), -0.2, 0.2)), 0.02, 0.2)
    remap_cell = set_ends(jax.random.randint(key_list[8], (TILES, TILES, CAP), 0, OCELLS), jax.random.fold_in(key_list[8], 1), 0, OCELLS - 1).astype(jnp.int32)
    fold_perm = draw_fold_perm(jax.random.fold_in(key_list[10], 71), 0)
    return dict(disc_pos=disc_pos, disc_vel=disc_vel, radius=radius, bond_list=bond_list, contact_mask=contact_mask, remap_block=remap_block, ocean_state=ocean_state, mix_coef=mix_coef, remap_cell=remap_cell, fold_perm=fold_perm)


SOFTEN = 0.0001
STIFFNESS = 2.0
BOND_STIFF = 0.1
TIME_STEP = 0.05
DRAG_ICE = 15.0
DRAG_BACK = 0.5
VERT_MIX = 0.1
SPIN_RATE = 0.3
ALL_SHIFTS = ((-1, -1), (-1, 0), (-1, 1), (0, -1), (0, 0), (0, 1), (1, -1), (1, 0), (1, 1))

def pair_force(own, other, shift_y, shift_x):
    sep_x = other[0][..., None, :] + shift_x - own[0][..., :, None]
    sep_y = other[1][..., None, :] + shift_y - own[1][..., :, None]
    distance = jnp.sqrt(sep_x * sep_x + sep_y * sep_y + SOFTEN)
    push = STIFFNESS * jnp.maximum(own[2][..., :, None] + other[2][..., None, :] - distance, 0.0) / distance
    return jnp.stack([-lax.optimization_barrier(jnp.sum(push * sep_x, axis=-1)), -lax.optimization_barrier(jnp.sum(push * sep_y, axis=-1))])

def make_weights(contact_mask):
    rows = jnp.arange(NBY, dtype=jnp.int32)
    masked = contact_mask.astype(jnp.float32)
    weights = []
    counter = 0
    for shift_y, shift_x in ALL_SHIFTS:
        if shift_y == 0 and shift_x == 0:
            weights.append(jnp.ones((NBY, NBX), jnp.float32))
        else:
            inside = ((rows + shift_y >= 0) & (rows + shift_y < NBY)).astype(jnp.float32)
            weights.append(masked[counter] * inside[:, None])
            counter = counter + 1
    return jnp.stack(weights)

def contact_all(state, weights):
    wide = jnp.concatenate([state[:, :, -1:], state, state[:, :, :1]], axis=2)
    wide = jnp.pad(wide, ((0, 0), (1, 1), (0, 0), (0, 0)))

    def one_row(inputs):
        row, weight_row = inputs
        band = lax.dynamic_slice_in_dim(wide, row, 3, axis=1)
        own = band[:, 1, 1:NBX + 1]
        total = jnp.zeros((2, NBX, own.shape[2]), jnp.float32)
        for index, (shift_y, shift_x) in enumerate(ALL_SHIFTS):
            other = band[:, 1 + shift_y, 1 + shift_x:1 + shift_x + NBX]
            total = total + pair_force(own, other, float(shift_y), float(shift_x)) * weight_row[index][None, :, None]
        return total
    rows = jnp.arange(NBY, dtype=jnp.int32)
    result = lax.map(one_row, (rows, jnp.moveaxis(weights, 1, 0)))
    return jnp.moveaxis(result, 0, 1)

def to_tiles(field):
    lead = field.shape[0]
    shaped = field.reshape(lead, N_GY, BGY, N_GX, BGX).transpose(0, 3, 1, 2, 4)
    return shaped.reshape(lead, TILES, BGY * BGX)

def from_tiles(field):
    lead = field.shape[0]
    shaped = field.reshape(lead, N_GX, N_GY, BGY, BGX).transpose(0, 2, 3, 1, 4)
    return shaped.reshape(lead, NBY, NBX)

def ocean_step(ocean_state, mix_coef, forcing, fold_perm):
    east = jnp.roll(ocean_state, -1, axis=3)
    west = jnp.roll(ocean_state, 1, axis=3)
    south = jnp.concatenate([jnp.zeros_like(ocean_state[:, :, :1]), ocean_state[:, :, :-1]], axis=2)
    signs = jnp.array([-1.0, -1.0, 1.0, 1.0], jnp.float32)[:, None, None]
    mirrored = signs * jnp.take(ocean_state[:, :, -1], fold_perm, axis=2)
    north = jnp.concatenate([ocean_state[:, :, 1:], mirrored[:, :, None]], axis=2)
    laplace = east + west + north + south - 4.0 * ocean_state
    above = jnp.concatenate([ocean_state[:, :1], ocean_state[:, :-1]], axis=1)
    below = jnp.concatenate([ocean_state[:, 1:], ocean_state[:, -1:]], axis=1)
    vertical = above + below - 2.0 * ocean_state
    updated = ocean_state + mix_coef[None] * laplace + VERT_MIX * vertical
    latitude = jnp.arange(NYO, dtype=jnp.float32)
    coriolis = (SPIN_RATE * (2.0 * (latitude + 0.5) / NYO - 1.0))[None, :, None]
    updated = updated.at[0].add(coriolis * ocean_state[1])
    updated = updated.at[1].add(-coriolis * ocean_state[0])
    updated = updated.at[0:2, 0].add(forcing)
    return updated

def reference(disc_pos, disc_vel, radius, bond_list, contact_mask, remap_block, ocean_state, mix_coef, remap_cell, fold_perm):
    mass = (radius / 0.06) ** 2
    weights = make_weights(contact_mask)
    position, velocity = (disc_pos, disc_vel)
    for substep in range(SUB):
        state = jnp.concatenate([position, radius[None]], axis=0)
        contact = contact_all(state, weights)
        bonded = jnp.stack([reduce_value(lambda left, right: left + right, [jnp.take_along_axis(position[comp], bond_list[partner], axis=-1) for partner in range(BONDS)]) for comp in range(2)])
        force = contact + BOND_STIFF * (bonded - BONDS * position)
        velocity = velocity + force / mass
        position = position + TIME_STEP * velocity
    impulse = DRAG_ICE * lax.optimization_barrier(jnp.sum(radius * radius * velocity, axis=-1))
    blocks = BGX * BGY
    tile_impulse = to_tiles(impulse)
    chosen = jnp.clip(remap_block, 0, blocks - 1).reshape(1, TILES, TILES * CAP)
    values = jnp.take_along_axis(tile_impulse, chosen, axis=2).reshape(2, TILES, TILES, CAP)
    values = jnp.where(remap_block[None] >= 0, values, 0.0).transpose(0, 2, 1, 3)
    tile_ids = jnp.arange(TILES, dtype=jnp.int32)
    segment_ids = (tile_ids[:, None, None] * OCELLS + remap_cell).reshape(-1)
    forcing = jax.ops.segment_sum(values.reshape(2, -1).T, segment_ids, num_segments=TILES * OCELLS).T
    forcing = forcing.reshape(2, N_GX, N_GY, OY, OX).transpose(0, 2, 3, 1, 4).reshape(2, NYO, NXO)
    ocean_next = ocean_step(ocean_state, mix_coef, forcing, fold_perm)
    surface = ocean_next[0:2, 0].reshape(2, N_GY, OY, N_GX, OX).transpose(0, 3, 1, 2, 4).reshape(2, TILES, OCELLS)
    current = jnp.take_along_axis(surface, remap_cell.reshape(1, TILES, TILES * CAP), axis=2)
    current = current.reshape(2, TILES, TILES, CAP).transpose(0, 2, 1, 3)
    block_ids = jnp.where(remap_block >= 0, tile_ids[:, None, None] * blocks + remap_block, TILES * blocks).reshape(-1)
    per_block = jax.ops.segment_sum(current.reshape(2, -1).T, block_ids, num_segments=TILES * blocks + 1)[:TILES * blocks].T
    per_block = from_tiles(per_block.reshape(2, TILES, blocks))
    vel_next = velocity + DRAG_BACK * (per_block[..., None] - velocity)
    return (position, vel_next, ocean_next)

def reduce_value(function, items):
    total = items[0]
    for item in items[1:]:
        total = function(total, item)
    return total
```

```python
import functools

import jax
import jax.numpy as jnp
import numpy as np
from jax import lax
from jax.experimental import pallas as pl
from jax.experimental.pallas import tpu as pltpu
from jax.sharding import PartitionSpec as P

BONDS = 4
SUB = 3


SOFTEN = 0.0001
STIFFNESS = 2.0
BOND_STIFF = 0.1
TIME_STEP = 0.05
DRAG_ICE = 15.0
DRAG_BACK = 0.5
VERT_MIX = 0.1
SPIN_RATE = 0.3
ALL_SHIFTS = ((-1, -1), (-1, 0), (-1, 1), (0, -1), (0, 0), (0, 1), (1, -1), (1, 0), (1, 1))
CENTER = 4
UNROLL = 16
DEPTH = 80
HIGHEST = lax.Precision.HIGHEST


def shift_tables():
    add = np.zeros((9, 32, 384), np.float32)
    scale = np.zeros((9, 32, 128), np.float32)
    for s, (sy, sx) in enumerate(ALL_SHIFTS):
        for g in (0, 8, 16):
            add[s, g, :128] = 2 * sx
            add[s, g + 1, :128] = 2 * sy
        add[s, 3, :128] = sx * sx + sy * sy
        add[s, 30, 128:256] = sx
        add[s, 30, 256:] = sy
        scale[s, 24:27] = -2 * sx
        scale[s, 27:30] = -2 * sy
    return add, scale


def pair_codes(rows, cols):
    own = rows * cols
    base_left, base_right = own, own + rows
    base_low = own + 2 * rows
    base_high = base_low + cols + 2
    code = np.zeros((own, 9), np.int32)
    for y in range(rows):
        for x in range(cols):
            for s, (sy, sx) in enumerate(ALL_SHIFTS):
                ny, nx = y + sy, x + sx
                if ny < 0:
                    j = base_low + nx + 1
                elif ny >= rows:
                    j = base_high + nx + 1
                elif nx < 0:
                    j = base_left + ny
                elif nx >= cols:
                    j = base_right + ny
                else:
                    j = ny * cols + nx
                code[y * cols + x, s] = ((y * cols + x) * 256 + j) * 16 + s
    return code.reshape(-1), base_high + cols + 2


def list_kernel(active_ref, code_ref, inner_ref, outer_ref, count_ref, *, own):
    def step(i, counts):
        inner, outer = counts
        others = 0
        for s in range(9):
            code = code_ref[i * 9 + s]
            inner_ref[inner] = code
            if s == CENTER:
                inner = inner + 1
                continue
            outer_ref[outer] = code
            flag = active_ref[others * own + i]
            away = (((code >> 4) & 255) >= own).astype(jnp.int32) * flag
            inner = inner + (flag - away)
            outer = outer + away
            others = others + 1
        return inner, outer

    inner, outer = lax.fori_loop(0, own, step, (jnp.int32(0), jnp.int32(0)))
    for u in range(UNROLL):
        inner_ref[inner + u] = jnp.int32((own * 256) * 16 + CENTER)
        outer_ref[outer + u] = jnp.int32((own * 256 + own) * 16 + CENTER)
    count_ref[0] = inner
    count_ref[1] = outer


def top_bits(value):
    scaled = value * 65537.0
    return scaled - (scaled - value)


def split(tile):
    high = top_bits(tile)
    rest = tile - high
    mid = top_bits(rest)
    return high, mid, rest - mid


def far_features(tile, at_ref, index):
    high, mid, low = split(tile)
    stack = [high, high, mid, mid, high, low, high, mid, low, jnp.ones((8, 128), jnp.float32)]
    at_ref[index] = jnp.concatenate(stack, axis=0).T.astype(jnp.bfloat16)
    return high, mid, low


def near_features(parts, head_ref, tail_ref, index):
    row_id = lax.broadcasted_iota(jnp.int32, (8, 128), 0)
    zero8 = jnp.zeros((8, 128), jnp.float32)
    dist_scale = jnp.where(row_id < 2, -2.0, jnp.where(row_id < 4, 1.0, 0.0))
    reach_scale = jnp.where((row_id == 4) | (row_id == 5), 1.0, 0.0)
    swap_up = (row_id == 3) | (row_id == 5)
    swap_down = (row_id == 2) | (row_id == 4)
    only_x = jnp.where(row_id == 0, 1.0, 0.0)
    only_y = jnp.where(row_id == 1, 1.0, 0.0)

    def swapped(tile):
        up = pltpu.roll(tile, 1, 0)
        down = pltpu.roll(tile, 7, 0)
        return jnp.where(swap_up, up, jnp.where(swap_down, down, tile))

    def gathered(row):
        rows = [jnp.broadcast_to(part[row : row + 1], (8, 128)) for part in parts]
        picked = jnp.where(row_id == 0, rows[0], jnp.where(row_id == 1, rows[1], rows[2]))
        return jnp.where(row_id < 3, picked, 0.0)

    high, mid, low = [swapped(part) for part in parts]
    order = [high, mid, high, mid, low, high]
    dist = jnp.concatenate([part * dist_scale for part in order], axis=0)
    reach = jnp.concatenate([part * reach_scale for part in order], axis=0)
    off_x = jnp.concatenate([only_x, zero8, only_x, zero8, zero8, only_x], axis=0)
    off_y = jnp.concatenate([only_y, zero8, only_y, zero8, zero8, only_y], axis=0)
    head_ref[index] = jnp.concatenate([dist, off_x, off_y, reach], axis=1).astype(jnp.bfloat16)
    first = gathered(0)
    second = gathered(1)
    both = first + pltpu.roll(second, 3, 0)
    zero24 = jnp.zeros((24, 384), jnp.float32)
    last = jnp.concatenate([both, -first, -second], axis=1)
    tail_ref[index] = jnp.concatenate([zero24, last], axis=0).astype(jnp.bfloat16)


def clear_spare(own, head_ref, tail_ref, acc_ref):
    head_ref[own] = jnp.zeros((48, 512), jnp.bfloat16)
    tail_ref[own] = jnp.zeros((32, 384), jnp.bfloat16)
    acc_ref[own] = jnp.zeros((16, 128), jnp.float32)


def visit(count, list_ref, far_base, at_ref, head_ref, tail_ref, add_ref, scale_ref, acc_ref):
    pad = jnp.zeros((32, 128), jnp.bfloat16)

    def pairs(step, carry):
        for u in range(UNROLL):
            code = list_ref[step * UNROLL + u]
            s = code & 15
            j = ((code >> 4) & 255) - far_base
            i = code >> 12
            tail = tail_ref[i]
            dist = tail[:, :128] * scale_ref[s]
            tail = jnp.concatenate([dist, tail[:, 128:]], axis=1) + add_ref[s]
            near = jnp.concatenate(
                [head_ref[i], jnp.concatenate([tail, pad], axis=1)], axis=0
            )
            every = jnp.dot(at_ref[j], near, preferred_element_type=jnp.float32)
            square = jnp.maximum(every[:, :128], SOFTEN)
            push = jnp.maximum(every[:, 384:] * lax.rsqrt(square) - 1.0, 0.0)
            sum_x = jnp.sum((push * every[:, 128:256]).reshape(16, 8, 128), axis=0)
            sum_y = jnp.sum((push * every[:, 256:384]).reshape(16, 8, 128), axis=0)
            acc_ref[i] = acc_ref[i] + jnp.concatenate([sum_x, sum_y], axis=0)
        return carry

    lax.fori_loop(0, (count + (UNROLL - 1)) // UNROLL, pairs, 0)


def inner_kernel(
    count_ref, list_ref, own_ref, add_ref, scale_ref, acc_ref, at_ref, head_ref, tail_ref
):
    own = own_ref.shape[0]

    def build(b, carry):
        parts = far_features(own_ref[b], at_ref, b)
        near_features(parts, head_ref, tail_ref, b)
        acc_ref[b] = jnp.zeros((16, 128), jnp.float32)
        return carry

    lax.fori_loop(0, own, build, 0, unroll=4)
    clear_spare(own, head_ref, tail_ref, acc_ref)
    visit(
        count_ref[0], list_ref, 0, at_ref, head_ref, tail_ref, add_ref, scale_ref, acc_ref
    )


def outer_kernel(
    count_ref,
    list_ref,
    own_ref,
    left_ref,
    right_ref,
    low_ref,
    high_ref,
    vel_ref,
    bond_ref,
    add_ref,
    scale_ref,
    inner_ref,
    next_ref,
    velnext_ref,
    at_ref,
    head_ref,
    tail_ref,
    acc_ref,
):
    own = own_ref.shape[0]
    rows = left_ref.shape[0]
    cols = own // rows

    def build(b):
        near_features(split(own_ref[b]), head_ref, tail_ref, b)

    def build_column(y, carry):
        build(y * cols)
        build(y * cols + cols - 1)
        return carry

    def build_row(x, carry):
        build(x)
        build((rows - 1) * cols + x)
        return carry

    lax.fori_loop(0, rows, build_column, 0, unroll=2)
    lax.fori_loop(1, cols - 1, build_row, 0, unroll=2)

    def clear(b, carry):
        acc_ref[b] = jnp.zeros((16, 128), jnp.float32)
        return carry

    lax.fori_loop(0, own, clear, 0, unroll=8)
    clear_spare(own, head_ref, tail_ref, acc_ref)
    base = 0
    for ref in (left_ref, right_ref, low_ref, high_ref):

        def build_halo(b, carry, ref=ref, base=base):
            far_features(ref[b], at_ref, base + b)
            return carry

        lax.fori_loop(0, ref.shape[0], build_halo, 0, unroll=2)
        base = base + ref.shape[0]
    visit(
        count_ref[1], list_ref, own, at_ref, head_ref, tail_ref, add_ref, scale_ref, acc_ref
    )
    row_id = lax.broadcasted_iota(jnp.int32, (8, 128), 0)

    def update(b, carry):
        tile = own_ref[b]
        vel = vel_ref[b]
        acc = acc_ref[b] + inner_ref[b]
        sum_x = jnp.sum(acc[:8], axis=0, keepdims=True)
        sum_y = jnp.sum(acc[8:], axis=0, keepdims=True)
        contact = -STIFFNESS * jnp.where(row_id == 0, sum_x, sum_y)
        bonded = -float(BONDS) * tile
        for partner in range(BONDS):
            index = jnp.broadcast_to(bond_ref[partner, pl.ds(b, 1), :], (8, 128))
            bonded = bonded + jnp.take_along_axis(
                tile, index, axis=1, mode="promise_in_bounds"
            )
        force = contact + BOND_STIFF * bonded
        over_mass = jnp.broadcast_to(vel[2:3], (8, 128))
        new_vel = vel + force * over_mass
        new_pos = tile + TIME_STEP * new_vel
        square = new_pos * new_pos
        length = pltpu.roll(square, 2, 0) + pltpu.roll(square, 1, 0) + 0.5 * SOFTEN
        next_ref[b] = jnp.where(row_id < 2, new_pos, jnp.where(row_id == 2, length, tile))
        velnext_ref[b] = jnp.where(row_id < 2, new_vel, vel)
        return carry

    lax.fori_loop(0, own, update, 0, unroll=4)


def smem():
    return pl.BlockSpec(memory_space=pltpu.MemorySpace.SMEM)


def vmem():
    return pl.BlockSpec(memory_space=pltpu.MemorySpace.VMEM)


def edge_kernel(ocean_ref, edge_ref, south_ref, north_ref, *, rows):
    total, lanes = ocean_ref.shape
    count = total // lanes
    lane = lax.broadcasted_iota(jnp.int32, (lanes, lanes), 1)
    wide = jnp.zeros((lanes, lanes), jnp.float32)
    for q in range(count):
        part = ocean_ref[q * lanes : (q + 1) * lanes, :]
        wide = jnp.where(lane == q, pltpu.roll(part, (q + 1) % lanes, 1), wide)
        wide = jnp.where(lane == lanes // 2 + q, pltpu.roll(part, lanes // 2 + q, 1), wide)
    edge_ref[...] = wide.T
    south_ref[...] = ocean_ref[pl.ds(0, total // rows, rows), :]
    north_ref[...] = ocean_ref[pl.ds(rows - 1, total // rows, rows), :]


def ocean_kernel(
    flags_ref,
    ocean_ref,
    before_ref,
    after_ref,
    mix_ref,
    west_ref,
    east_ref,
    south_ref,
    north_ref,
    top_ref,
    perm_ref,
    cor_ref,
    out_ref,
    fold_ref,
    wcol_ref,
    ecol_ref,
):
    fields, chunk, rows, lanes = ocean_ref.shape
    layers = south_ref.shape[0] // fields
    planes = fields * layers

    @pl.when(pl.program_id(0) == 0)
    def _():
        columns = jnp.broadcast_to(perm_ref[...], (planes, lanes))
        mirrored = jnp.zeros((planes, lanes), jnp.float32)
        for source in range(top_ref.shape[0]):
            picked = jnp.take_along_axis(
                top_ref[source], columns & (lanes - 1), axis=1, mode="promise_in_bounds"
            )
            mirrored = jnp.where(columns // lanes == source, picked, mirrored)
        plane_id = lax.broadcasted_iota(jnp.int32, (planes, lanes), 0)
        mirrored = jnp.where(plane_id < 2 * layers, -mirrored, mirrored)
        fold_ref[...] = jnp.where(flags_ref[0] > 0, mirrored, north_ref[...])
        pad = jnp.zeros((lanes - west_ref.shape[0], lanes), jnp.float32)
        wcol_ref[...] = jnp.concatenate([west_ref[...], pad], axis=0).T
        ecol_ref[...] = jnp.concatenate([east_ref[...], pad], axis=0).T

    per = lanes // rows
    lane = lax.broadcasted_iota(jnp.int32, (rows, lanes), 1)
    row = lax.broadcasted_iota(jnp.int32, (rows, lanes), 0)
    cor = cor_ref[...]
    for local in range(chunk):
        k = pl.program_id(0) * chunk + local
        mix = mix_ref[local]
        old = [ocean_ref[f, local] for f in range(fields)]
        for f in range(fields):
            here = old[f]
            plane = f * layers + k
            place = jnp.full((rows, lanes), plane // per, jnp.int32)
            start = pl.multiple_of((plane % per) * rows, 8)
            wcol = jnp.take_along_axis(
                wcol_ref[pl.ds(start, rows), :], place, axis=1, mode="promise_in_bounds"
            )
            ecol = jnp.take_along_axis(
                ecol_ref[pl.ds(start, rows), :], place, axis=1, mode="promise_in_bounds"
            )
            west = jnp.where(lane == 0, wcol, pltpu.roll(here, 1, 1))
            east = jnp.where(lane == lanes - 1, ecol, pltpu.roll(here, lanes - 1, 1))
            below_row = jnp.broadcast_to(south_ref[pl.ds(plane, 1), :], (rows, lanes))
            above_row = jnp.broadcast_to(fold_ref[pl.ds(plane, 1), :], (rows, lanes))
            south = jnp.where(row == 0, below_row, pltpu.roll(here, 1, 0))
            north = jnp.where(row == rows - 1, above_row, pltpu.roll(here, rows - 1, 0))
            laplace = east + west + north + south - 4.0 * here
            above = before_ref[f, 0] if local == 0 else ocean_ref[f, local - 1]
            below = after_ref[f, 0] if local == chunk - 1 else ocean_ref[f, local + 1]
            vertical = above + below - 2.0 * here
            new = here + mix * laplace + VERT_MIX * vertical
            if f == 0:
                new = new + cor * old[1]
            elif f == 1:
                new = new - cor * old[0]
            out_ref[f, local] = new


def ring(axis, step):
    count = lax.axis_size(axis)
    return [(i, (i + step) % count) for i in range(count)]


def line(axis, step):
    count = lax.axis_size(axis)
    return [(i, i + step) for i in range(count) if 0 <= i + step < count]


def halos(state):
    rows, cols = state.shape[:2]
    left = lax.ppermute(state[:, cols - 1], "gx", ring("gx", 1))
    right = lax.ppermute(state[:, 0], "gx", ring("gx", -1))
    bottom = jnp.concatenate([left[:1], state[0], right[:1]], axis=0)
    top = jnp.concatenate([left[rows - 1 :], state[rows - 1], right[rows - 1 :]], axis=0)
    state, bottom, top = lax.optimization_barrier((state, bottom, top))
    low = lax.ppermute(top, "gy", line("gy", 1))
    high = lax.ppermute(bottom, "gy", line("gy", -1))
    return state, left, right, low, high


def body(
    disc_pos,
    disc_vel,
    radius,
    bond_list,
    contact_mask,
    remap_block,
    ocean_state,
    mix_coef,
    remap_cell,
    fold_perm,
):
    rows_dev, cols_dev, disc_count = radius.shape
    block_count = rows_dev * cols_dev
    lat_tiles = lax.axis_size("gy")
    total_rows = rows_dev * lat_tiles
    _, tile_count, capacity = remap_block.shape
    slots = tile_count * capacity
    fields, layers, tile_rows, tile_cols = ocean_state.shape
    planes = fields * layers
    f32 = jnp.float32

    edge_rows = tile_cols // 2
    edges, south_row, north_row = pl.pallas_call(
        functools.partial(edge_kernel, rows=tile_rows),
        out_shape=(
            jax.ShapeDtypeStruct((tile_cols, tile_cols), f32),
            jax.ShapeDtypeStruct((planes, tile_cols), f32),
            jax.ShapeDtypeStruct((planes, tile_cols), f32),
        ),
        cost_estimate=pl.CostEstimate(flops=10**7, transcendentals=0, bytes_accessed=4 * 10**6),
        name="edges",
    )(ocean_state.reshape(planes * tile_rows, tile_cols))
    west = lax.ppermute(edges[:edge_rows], "gx", ring("gx", 1))
    east = lax.ppermute(edges[edge_rows:], "gx", ring("gx", -1))
    from_south = lax.ppermute(north_row, "gy", line("gy", 1))
    from_north = lax.ppermute(south_row, "gy", line("gy", -1))
    lon_tiles = lax.axis_size("gx")
    tops = lax.all_to_all(
        jnp.broadcast_to(north_row[None], (lon_tiles, planes, tile_cols)),
        "gx",
        split_axis=0,
        concat_axis=0,
        tiled=True,
    )

    global_rows = lax.axis_index("gy") * rows_dev + jnp.arange(rows_dev, dtype=jnp.int32)
    shift_rows = jnp.asarray([sy for sy, sx in ALL_SHIFTS if (sy, sx) != (0, 0)], jnp.int32)
    other_rows = shift_rows[:, None] + global_rows[None]
    inside = (other_rows >= 0) & (other_rows < total_rows)
    active = jnp.where(inside[:, :, None], contact_mask, 0).reshape(-1)
    codes, wide_count = pair_codes(rows_dev, cols_dev)
    list_shape = jax.ShapeDtypeStruct((block_count * 9 + UNROLL,), jnp.int32)
    inner_list, outer_list, pair_count = pl.pallas_call(
        functools.partial(list_kernel, own=block_count),
        in_specs=[smem(), smem()],
        out_specs=(smem(), smem(), smem()),
        out_shape=(list_shape, list_shape, jax.ShapeDtypeStruct((2,), jnp.int32)),
        cost_estimate=pl.CostEstimate(flops=10**7, transcendentals=0, bytes_accessed=10**4),
        name="pairlist",
    )(active, jnp.asarray(codes))

    add_np, scale_np = shift_tables()
    add_tab = jnp.asarray(add_np, jnp.bfloat16)
    scale_tab = jnp.asarray(scale_np, jnp.bfloat16)

    ones = jnp.ones_like(radius)
    zeros = jnp.zeros_like(radius)
    length = disc_pos[0] * disc_pos[0] + disc_pos[1] * disc_pos[1] + 0.5 * SOFTEN
    state = jnp.stack([disc_pos[0], disc_pos[1], length, ones, radius, ones, zeros, zeros], axis=2)
    over_mass = 1.0 / ((radius / 0.06) ** 2)
    vel = jnp.stack([disc_vel[0], disc_vel[1], over_mass] + [zeros] * 5, axis=2)
    vel = vel.reshape(block_count, 8, disc_count)
    bonds = bond_list.reshape(BONDS, block_count, disc_count)
    near_scratch = [
        pltpu.VMEM((block_count + 1, 48, 4 * disc_count), jnp.bfloat16),
        pltpu.VMEM((block_count + 1, 32, 3 * disc_count), jnp.bfloat16),
    ]
    acc_shape = (block_count + 1, 16, disc_count)

    def substep(state, vel):
        state, left, right, low, high = halos(state)
        own = state.reshape(block_count, 8, disc_count)
        inner = pl.pallas_call(
            inner_kernel,
            in_specs=[smem(), smem()] + [vmem()] * 3,
            out_specs=vmem(),
            out_shape=jax.ShapeDtypeStruct(acc_shape, f32),
            scratch_shapes=[pltpu.VMEM((block_count, disc_count, DEPTH), jnp.bfloat16)]
            + near_scratch,
            cost_estimate=pl.CostEstimate(
                flops=8 * 10**9, transcendentals=10**7, bytes_accessed=2 * 10**6
            ),
            name="inner",
        )(pair_count, inner_list, own, add_tab, scale_tab)
        own, vel = pl.pallas_call(
            outer_kernel,
            in_specs=[smem(), smem()] + [vmem()] * 10,
            out_specs=(vmem(), vmem()),
            out_shape=(
                jax.ShapeDtypeStruct(own.shape, f32),
                jax.ShapeDtypeStruct(own.shape, f32),
            ),
            scratch_shapes=[
                pltpu.VMEM((wide_count - block_count + 1, disc_count, DEPTH), jnp.bfloat16)
            ]
            + near_scratch
            + [pltpu.VMEM(acc_shape, f32)],
            cost_estimate=pl.CostEstimate(
                flops=10**9, transcendentals=10**6, bytes_accessed=4 * 10**6
            ),
            name="outer",
        )(
            pair_count,
            outer_list,
            own,
            left,
            right,
            low,
            high,
            vel,
            bonds,
            add_tab,
            scale_tab,
            inner,
        )
        return own.reshape(rows_dev, cols_dev, 8, disc_count), vel

    state, vel = substep(state, vel)
    state, west, east, from_south, from_north, tops = lax.optimization_barrier(
        (state, west, east, from_south, from_north, tops)
    )

    is_top = (lax.axis_index("gy") == lat_tiles - 1).astype(jnp.int32).reshape(1)
    latitude = (lax.axis_index("gy") * tile_rows + jnp.arange(tile_rows, dtype=jnp.int32)).astype(
        f32
    )
    coriolis = SPIN_RATE * (2.0 * (latitude + 0.5) / (tile_rows * lat_tiles) - 1.0)
    coriolis = jnp.broadcast_to(coriolis[:, None], (tile_rows, tile_cols))
    chunk = next(size for size in (6, 4, 3, 2, 1) if layers % size == 0)

    def whole(shape):
        return pl.BlockSpec(shape, lambda g: (0,) * len(shape))

    def layer_block(size, index):
        return pl.BlockSpec(
            (fields, size, tile_rows, tile_cols), lambda g: (0, index(g), 0, 0)
        )

    updated = pl.pallas_call(
        ocean_kernel,
        grid=(layers // chunk,),
        in_specs=[
            smem(),
            layer_block(chunk, lambda g: g),
            layer_block(1, lambda g: jnp.maximum(g * chunk - 1, 0)),
            layer_block(1, lambda g: jnp.minimum(g * chunk + chunk, layers - 1)),
            pl.BlockSpec((chunk, tile_rows, tile_cols), lambda g: (g, 0, 0)),
            whole(west.shape),
            whole(east.shape),
            whole(from_south.shape),
            whole(from_north.shape),
            whole(tops.shape),
            whole((1, tile_cols)),
            whole(coriolis.shape),
        ],
        out_specs=layer_block(chunk, lambda g: g),
        out_shape=jax.ShapeDtypeStruct(ocean_state.shape, f32),
        scratch_shapes=[
            pltpu.VMEM((planes, tile_cols), f32),
            pltpu.VMEM((tile_cols, tile_cols), f32),
            pltpu.VMEM((tile_cols, tile_cols), f32),
        ],
        cost_estimate=pl.CostEstimate(flops=10**8, transcendentals=0, bytes_accessed=7 * 10**6),
        name="ocean",
    )(
        is_top,
        ocean_state,
        ocean_state,
        ocean_state,
        mix_coef,
        west,
        east,
        from_south,
        from_north,
        tops,
        fold_perm.reshape(1, tile_cols),
        coriolis,
    )

    cells = remap_cell[0].reshape(-1)
    surface = updated[0:2, 0].reshape(2, tile_rows * tile_cols)
    unforced = jnp.take(surface, cells, axis=1).reshape(2, tile_count, capacity)
    early = jnp.concatenate(
        [
            jnp.broadcast_to(cells.astype(f32)[None], (tile_count, slots)),
            unforced.transpose(1, 0, 2).reshape(tile_count, 2 * capacity),
        ],
        axis=1,
    )
    early = lax.all_to_all(early, ("gx", "gy"), split_axis=0, concat_axis=0, tiled=True)
    for step in range(1, SUB):
        state, vel = substep(state, vel)
        if step == 1:
            state, early = lax.optimization_barrier((state, early))
    all_cells = early[:, :slots].reshape(tile_count, tile_count, capacity)
    unforced = early[:, slots:].reshape(tile_count, 2, capacity)

    vel_rows = vel[:, 0:2]
    weight = radius.reshape(block_count, 1, disc_count) ** 2
    impulse = DRAG_ICE * jnp.sum(weight * vel_rows, axis=-1)
    selector = (
        remap_block[0].reshape(-1)[:, None] == jnp.arange(block_count, dtype=jnp.int32)[None]
    ).astype(f32)
    outgoing = lax.dot_general(
        impulse, selector, (((0,), (1,)), ((), ())), precision=HIGHEST
    ).reshape(1, 2 * slots)
    arrived = lax.all_to_all(
        jnp.broadcast_to(outgoing, (tile_count, 2 * slots)),
        ("gx", "gy"),
        split_axis=0,
        concat_axis=0,
        tiled=True,
    ).reshape(tile_count, 2, tile_count, capacity)

    tile_id = lax.axis_index("gx") * lat_tiles + lax.axis_index("gy")
    mine = lax.dynamic_index_in_dim(all_cells, tile_id, axis=1, keepdims=False)
    same = all_cells[:, None] == mine[:, :, None, None]
    landed = arrived.transpose(1, 2, 0, 3)
    forced = jnp.sum(jnp.where(same[None], landed[:, :, None], 0.0), axis=(3, 4))
    current = unforced.transpose(1, 0, 2) + forced
    per_block = jnp.dot(current.reshape(2, slots), selector, precision=HIGHEST)
    per_block = per_block.reshape(2, rows_dev, cols_dev)
    velocity = vel.reshape(rows_dev, cols_dev, 8, disc_count)[:, :, 0:2].transpose(2, 0, 1, 3)
    position = state[:, :, 0:2].transpose(2, 0, 1, 3)
    vel_next = velocity + DRAG_BACK * (per_block[..., None] - velocity)

    here = lax.dynamic_index_in_dim(arrived, tile_id, axis=2, keepdims=False)
    here = here.transpose(1, 0, 2).reshape(2, 1, slots)
    in_row = (cells // tile_cols)[None] == jnp.arange(tile_rows, dtype=jnp.int32)[:, None]
    in_col = (cells % tile_cols)[:, None] == jnp.arange(tile_cols, dtype=jnp.int32)[None]
    forcing = jnp.dot(
        jnp.where(in_row[None], here, 0.0).reshape(2 * tile_rows, slots),
        in_col.astype(f32),
        precision=HIGHEST,
    ).reshape(2, tile_rows, tile_cols)
    updated = updated.at[0:2, 0].add(forcing)
    return (position, vel_next, updated)


def solution(mesh):
    in_specs = (
        P(None, "gy", "gx", None),
        P(None, "gy", "gx", None),
        P("gy", "gx", None),
        P(None, "gy", "gx", None),
        P(None, "gy", "gx"),
        P(("gx", "gy"), None, None),
        P(None, None, "gy", "gx"),
        P(None, "gy", "gx"),
        P(("gx", "gy"), None, None),
        P("gx"),
    )
    out_specs = (P(None, "gy", "gx", None), P(None, "gy", "gx", None), P(None, None, "gy", "gx"))
    return jax.shard_map(body, mesh=mesh, in_specs=in_specs, out_specs=out_specs, check_vma=False)
```

```python
import functools

import jax
import jax.numpy as jnp
import numpy as np
from jax import lax
from jax.experimental import pallas as pl
from jax.experimental.pallas import tpu as pltpu
from jax.sharding import PartitionSpec as P

BONDS = 4
SUB = 3


SOFTEN = 0.0001
STIFFNESS = 2.0
BOND_STIFF = 0.1
TIME_STEP = 0.05
DRAG_ICE = 15.0
DRAG_BACK = 0.5
VERT_MIX = 0.1
SPIN_RATE = 0.3
ALL_SHIFTS = ((-1, -1), (-1, 0), (-1, 1), (0, -1), (0, 0), (0, 1), (1, -1), (1, 0), (1, 1))
CENTER = 4
UNROLL = 32
OUTER_UNROLL = 16
DEPTH = 80
HIGHEST = lax.Precision.HIGHEST


def shift_tables():
    add = np.zeros((9, 32, 384), np.float32)
    scale = np.zeros((9, 32, 128), np.float32)
    for s, (sy, sx) in enumerate(ALL_SHIFTS):
        for g in (0, 8, 16):
            add[s, g, :128] = 2 * sx
            add[s, g + 1, :128] = 2 * sy
        add[s, 3, :128] = sx * sx + sy * sy
        add[s, 30, 128:256] = sx
        add[s, 30, 256:] = sy
        scale[s, 24:27] = -2 * sx
        scale[s, 27:30] = -2 * sy
    return add, scale


def pair_codes(rows, cols):
    own = rows * cols
    base_left, base_right = own, own + rows
    base_low = own + 2 * rows
    base_high = base_low + cols + 2
    code = np.zeros((own, 9), np.int32)
    for y in range(rows):
        for x in range(cols):
            for s, (sy, sx) in enumerate(ALL_SHIFTS):
                ny, nx = y + sy, x + sx
                if ny < 0:
                    j = base_low + nx + 1
                elif ny >= rows:
                    j = base_high + nx + 1
                elif nx < 0:
                    j = base_left + ny
                elif nx >= cols:
                    j = base_right + ny
                else:
                    j = ny * cols + nx
                code[y * cols + x, s] = ((y * cols + x) * 256 + j) * 16 + s
    return code.reshape(-1), base_high + cols + 2


def list_kernel(active_ref, code_ref, inner_ref, outer_ref, count_ref, *, own):
    def step(i, counts):
        inner, outer = counts
        others = 0
        for s in range(9):
            code = code_ref[i * 9 + s]
            inner_ref[inner] = code
            if s == CENTER:
                inner = inner + 1
                continue
            outer_ref[outer] = code
            flag = active_ref[others * own + i]
            away = (((code >> 4) & 255) >= own).astype(jnp.int32) * flag
            inner = inner + (flag - away)
            outer = outer + away
            others = others + 1
        return inner, outer

    inner, outer = lax.fori_loop(0, own, step, (jnp.int32(0), jnp.int32(0)))
    for u in range(UNROLL):
        inner_ref[inner + u] = jnp.int32((own * 256) * 16 + CENTER)
        outer_ref[outer + u] = jnp.int32((own * 256 + own) * 16 + CENTER)
    count_ref[0] = inner
    count_ref[1] = outer


def top_bits(value):
    scaled = value * 65537.0
    return scaled - (scaled - value)


def split(tile):
    high = top_bits(tile)
    rest = tile - high
    mid = top_bits(rest)
    return high, mid, rest - mid


def far_features(tile, at_ref, index):
    high, mid, low = split(tile)
    stack = [high, high, mid, mid, high, low, high, mid, low, jnp.ones((8, 128), jnp.float32)]
    at_ref[index] = jnp.concatenate(stack, axis=0).T.astype(jnp.bfloat16)
    return high, mid, low


def near_features(parts, head_ref, tail_ref, index):
    row_id = lax.broadcasted_iota(jnp.int32, (8, 128), 0)
    zero8 = jnp.zeros((8, 128), jnp.float32)
    dist_scale = jnp.where(row_id < 2, -2.0, jnp.where(row_id < 4, 1.0, 0.0))
    reach_scale = jnp.where((row_id == 4) | (row_id == 5), 1.0, 0.0)
    swap_up = (row_id == 3) | (row_id == 5)
    swap_down = (row_id == 2) | (row_id == 4)
    only_x = jnp.where(row_id == 0, 1.0, 0.0)
    only_y = jnp.where(row_id == 1, 1.0, 0.0)

    def swapped(tile):
        up = pltpu.roll(tile, 1, 0)
        down = pltpu.roll(tile, 7, 0)
        return jnp.where(swap_up, up, jnp.where(swap_down, down, tile))

    def gathered(row):
        rows = [jnp.broadcast_to(part[row : row + 1], (8, 128)) for part in parts]
        picked = jnp.where(row_id == 0, rows[0], jnp.where(row_id == 1, rows[1], rows[2]))
        return jnp.where(row_id < 3, picked, 0.0)

    high, mid, low = [swapped(part) for part in parts]
    order = [high, mid, high, mid, low, high]
    dist = jnp.concatenate([part * dist_scale for part in order], axis=0)
    reach = jnp.concatenate([part * reach_scale for part in order], axis=0)
    off_x = jnp.concatenate([only_x, zero8, only_x, zero8, zero8, only_x], axis=0)
    off_y = jnp.concatenate([only_y, zero8, only_y, zero8, zero8, only_y], axis=0)
    head_ref[index] = jnp.concatenate([dist, off_x, off_y, reach], axis=1).astype(jnp.bfloat16)
    first = gathered(0)
    second = gathered(1)
    both = first + pltpu.roll(second, 3, 0)
    zero24 = jnp.zeros((24, 384), jnp.float32)
    last = jnp.concatenate([both, -first, -second], axis=1)
    tail_ref[index] = jnp.concatenate([zero24, last], axis=0).astype(jnp.bfloat16)


def clear_spare(own, head_ref, tail_ref, acc_ref):
    head_ref[own] = jnp.zeros((48, 512), jnp.bfloat16)
    tail_ref[own] = jnp.zeros((32, 384), jnp.bfloat16)
    acc_ref[own] = jnp.zeros((16, 128), jnp.float32)


def visit(
    count, list_ref, far_base, at_ref, head_ref, tail_ref, add_ref, scale_ref, acc_ref, unroll
):
    pad = jnp.zeros((32, 128), jnp.bfloat16)

    def pairs(step, carry):
        for u in range(unroll):
            code = list_ref[step * unroll + u]
            s = code & 15
            j = ((code >> 4) & 255) - far_base
            i = code >> 12
            tail = tail_ref[i]
            dist = tail[:, :128] * scale_ref[s]
            tail = jnp.concatenate([dist, tail[:, 128:]], axis=1) + add_ref[s]
            near = jnp.concatenate(
                [head_ref[i], jnp.concatenate([tail, pad], axis=1)], axis=0
            )
            every = jnp.dot(at_ref[j], near, preferred_element_type=jnp.float32)
            square = jnp.maximum(every[:, :128], SOFTEN)
            push = jnp.maximum(every[:, 384:] * lax.rsqrt(square) - 1.0, 0.0)
            sum_x = jnp.sum((push * every[:, 128:256]).reshape(16, 8, 128), axis=0)
            sum_y = jnp.sum((push * every[:, 256:384]).reshape(16, 8, 128), axis=0)
            acc_ref[i] = acc_ref[i] + jnp.concatenate([sum_x, sum_y], axis=0)
        return carry

    lax.fori_loop(0, (count + (unroll - 1)) // unroll, pairs, 0)


def inner_kernel(
    count_ref, list_ref, own_ref, add_ref, scale_ref, acc_ref, at_ref, head_ref, tail_ref
):
    own = own_ref.shape[0]

    def build(b, carry):
        parts = far_features(own_ref[b], at_ref, b)
        near_features(parts, head_ref, tail_ref, b)
        acc_ref[b] = jnp.zeros((16, 128), jnp.float32)
        return carry

    lax.fori_loop(0, own, build, 0, unroll=4)
    clear_spare(own, head_ref, tail_ref, acc_ref)
    visit(
        count_ref[0], list_ref, 0, at_ref, head_ref, tail_ref, add_ref, scale_ref, acc_ref, UNROLL
    )


def outer_kernel(
    count_ref,
    list_ref,
    own_ref,
    left_ref,
    right_ref,
    low_ref,
    high_ref,
    vel_ref,
    bond_ref,
    add_ref,
    scale_ref,
    inner_ref,
    next_ref,
    velnext_ref,
    at_ref,
    head_ref,
    tail_ref,
    acc_ref,
):
    own = own_ref.shape[0]
    rows = left_ref.shape[0]
    cols = own // rows

    def build(b):
        near_features(split(own_ref[b]), head_ref, tail_ref, b)

    def build_column(y, carry):
        build(y * cols)
        build(y * cols + cols - 1)
        return carry

    def build_row(x, carry):
        build(x)
        build((rows - 1) * cols + x)
        return carry

    lax.fori_loop(0, rows, build_column, 0, unroll=2)
    lax.fori_loop(1, cols - 1, build_row, 0, unroll=2)

    def clear(b, carry):
        acc_ref[b] = jnp.zeros((16, 128), jnp.float32)
        return carry

    lax.fori_loop(0, own, clear, 0, unroll=8)
    clear_spare(own, head_ref, tail_ref, acc_ref)
    base = 0
    for ref in (left_ref, right_ref, low_ref, high_ref):

        def build_halo(b, carry, ref=ref, base=base):
            far_features(ref[b], at_ref, base + b)
            return carry

        lax.fori_loop(0, ref.shape[0], build_halo, 0, unroll=2)
        base = base + ref.shape[0]
    visit(
        count_ref[1],
        list_ref,
        own,
        at_ref,
        head_ref,
        tail_ref,
        add_ref,
        scale_ref,
        acc_ref,
        OUTER_UNROLL,
    )
    row_id = lax.broadcasted_iota(jnp.int32, (8, 128), 0)

    def update(b, carry):
        tile = own_ref[b]
        vel = vel_ref[b]
        acc = acc_ref[b] + inner_ref[b]
        sum_x = jnp.sum(acc[:8], axis=0, keepdims=True)
        sum_y = jnp.sum(acc[8:], axis=0, keepdims=True)
        contact = -STIFFNESS * jnp.where(row_id == 0, sum_x, sum_y)
        bonded = -float(BONDS) * tile
        for partner in range(BONDS):
            index = jnp.broadcast_to(bond_ref[partner, pl.ds(b, 1), :], (8, 128))
            bonded = bonded + jnp.take_along_axis(
                tile, index, axis=1, mode="promise_in_bounds"
            )
        force = contact + BOND_STIFF * bonded
        over_mass = jnp.broadcast_to(vel[2:3], (8, 128))
        new_vel = vel + force * over_mass
        new_pos = tile + TIME_STEP * new_vel
        square = new_pos * new_pos
        length = pltpu.roll(square, 2, 0) + pltpu.roll(square, 1, 0) + 0.5 * SOFTEN
        next_ref[b] = jnp.where(row_id < 2, new_pos, jnp.where(row_id == 2, length, tile))
        velnext_ref[b] = jnp.where(row_id < 2, new_vel, vel)
        return carry

    lax.fori_loop(0, own, update, 0, unroll=4)


def smem():
    return pl.BlockSpec(memory_space=pltpu.MemorySpace.SMEM)


def vmem():
    return pl.BlockSpec(memory_space=pltpu.MemorySpace.VMEM)


def edge_kernel(ocean_ref, edge_ref, south_ref, north_ref, *, rows):
    total, lanes = ocean_ref.shape
    count = total // lanes
    lane = lax.broadcasted_iota(jnp.int32, (lanes, lanes), 1)
    wide = jnp.zeros((lanes, lanes), jnp.float32)
    for q in range(count):
        part = ocean_ref[q * lanes : (q + 1) * lanes, :]
        wide = jnp.where(lane == q, pltpu.roll(part, (q + 1) % lanes, 1), wide)
        wide = jnp.where(lane == lanes // 2 + q, pltpu.roll(part, lanes // 2 + q, 1), wide)
    edge_ref[...] = wide.T
    south_ref[...] = ocean_ref[pl.ds(0, total // rows, rows), :]
    north_ref[...] = ocean_ref[pl.ds(rows - 1, total // rows, rows), :]


def ocean_kernel(
    flags_ref,
    ocean_ref,
    before_ref,
    after_ref,
    mix_ref,
    west_ref,
    east_ref,
    south_ref,
    north_ref,
    top_ref,
    perm_ref,
    cor_ref,
    out_ref,
    fold_ref,
    wcol_ref,
    ecol_ref,
):
    fields, chunk, rows, lanes = ocean_ref.shape
    layers = south_ref.shape[0] // fields
    planes = fields * layers

    @pl.when(pl.program_id(0) == 0)
    def _():
        columns = jnp.broadcast_to(perm_ref[...], (planes, lanes))
        mirrored = jnp.zeros((planes, lanes), jnp.float32)
        for source in range(top_ref.shape[0]):
            picked = jnp.take_along_axis(
                top_ref[source], columns & (lanes - 1), axis=1, mode="promise_in_bounds"
            )
            mirrored = jnp.where(columns // lanes == source, picked, mirrored)
        plane_id = lax.broadcasted_iota(jnp.int32, (planes, lanes), 0)
        mirrored = jnp.where(plane_id < 2 * layers, -mirrored, mirrored)
        fold_ref[...] = jnp.where(flags_ref[0] > 0, mirrored, north_ref[...])
        pad = jnp.zeros((lanes - west_ref.shape[0], lanes), jnp.float32)
        wcol_ref[...] = jnp.concatenate([west_ref[...], pad], axis=0).T
        ecol_ref[...] = jnp.concatenate([east_ref[...], pad], axis=0).T

    per = lanes // rows
    lane = lax.broadcasted_iota(jnp.int32, (rows, lanes), 1)
    row = lax.broadcasted_iota(jnp.int32, (rows, lanes), 0)
    cor = cor_ref[...]
    for local in range(chunk):
        k = pl.program_id(0) * chunk + local
        mix = mix_ref[local]
        old = [ocean_ref[f, local] for f in range(fields)]
        for f in range(fields):
            here = old[f]
            plane = f * layers + k
            place = jnp.full((rows, lanes), plane // per, jnp.int32)
            start = pl.multiple_of((plane % per) * rows, 8)
            wcol = jnp.take_along_axis(
                wcol_ref[pl.ds(start, rows), :], place, axis=1, mode="promise_in_bounds"
            )
            ecol = jnp.take_along_axis(
                ecol_ref[pl.ds(start, rows), :], place, axis=1, mode="promise_in_bounds"
            )
            west = jnp.where(lane == 0, wcol, pltpu.roll(here, 1, 1))
            east = jnp.where(lane == lanes - 1, ecol, pltpu.roll(here, lanes - 1, 1))
            below_row = jnp.broadcast_to(south_ref[pl.ds(plane, 1), :], (rows, lanes))
            above_row = jnp.broadcast_to(fold_ref[pl.ds(plane, 1), :], (rows, lanes))
            south = jnp.where(row == 0, below_row, pltpu.roll(here, 1, 0))
            north = jnp.where(row == rows - 1, above_row, pltpu.roll(here, rows - 1, 0))
            laplace = east + west + north + south - 4.0 * here
            above = before_ref[f, 0] if local == 0 else ocean_ref[f, local - 1]
            below = after_ref[f, 0] if local == chunk - 1 else ocean_ref[f, local + 1]
            vertical = above + below - 2.0 * here
            new = here + mix * laplace + VERT_MIX * vertical
            if f == 0:
                new = new + cor * old[1]
            elif f == 1:
                new = new - cor * old[0]
            out_ref[f, local] = new


def ring(axis, step):
    count = lax.axis_size(axis)
    return [(i, (i + step) % count) for i in range(count)]


def line(axis, step):
    count = lax.axis_size(axis)
    return [(i, i + step) for i in range(count) if 0 <= i + step < count]


def halos(state):
    rows, cols = state.shape[:2]
    left = lax.ppermute(state[:, cols - 1], "gx", ring("gx", 1))
    right = lax.ppermute(state[:, 0], "gx", ring("gx", -1))
    bottom = jnp.concatenate([left[:1], state[0], right[:1]], axis=0)
    top = jnp.concatenate([left[rows - 1 :], state[rows - 1], right[rows - 1 :]], axis=0)
    state, bottom, top = lax.optimization_barrier((state, bottom, top))
    low = lax.ppermute(top, "gy", line("gy", 1))
    high = lax.ppermute(bottom, "gy", line("gy", -1))
    return state, left, right, low, high


def body(
    disc_pos,
    disc_vel,
    radius,
    bond_list,
    contact_mask,
    remap_block,
    ocean_state,
    mix_coef,
    remap_cell,
    fold_perm,
):
    rows_dev, cols_dev, disc_count = radius.shape
    block_count = rows_dev * cols_dev
    lat_tiles = lax.axis_size("gy")
    total_rows = rows_dev * lat_tiles
    _, tile_count, capacity = remap_block.shape
    slots = tile_count * capacity
    fields, layers, tile_rows, tile_cols = ocean_state.shape
    planes = fields * layers
    f32 = jnp.float32

    edge_rows = tile_cols // 2
    edges, south_row, north_row = pl.pallas_call(
        functools.partial(edge_kernel, rows=tile_rows),
        out_shape=(
            jax.ShapeDtypeStruct((tile_cols, tile_cols), f32),
            jax.ShapeDtypeStruct((planes, tile_cols), f32),
            jax.ShapeDtypeStruct((planes, tile_cols), f32),
        ),
        cost_estimate=pl.CostEstimate(flops=10**7, transcendentals=0, bytes_accessed=4 * 10**6),
        name="edges",
    )(ocean_state.reshape(planes * tile_rows, tile_cols))
    west = lax.ppermute(edges[:edge_rows], "gx", ring("gx", 1))
    east = lax.ppermute(edges[edge_rows:], "gx", ring("gx", -1))
    from_south = lax.ppermute(north_row, "gy", line("gy", 1))
    from_north = lax.ppermute(south_row, "gy", line("gy", -1))
    lon_tiles = lax.axis_size("gx")
    tops = lax.all_to_all(
        jnp.broadcast_to(north_row[None], (lon_tiles, planes, tile_cols)),
        "gx",
        split_axis=0,
        concat_axis=0,
        tiled=True,
    )

    global_rows = lax.axis_index("gy") * rows_dev + jnp.arange(rows_dev, dtype=jnp.int32)
    shift_rows = jnp.asarray([sy for sy, sx in ALL_SHIFTS if (sy, sx) != (0, 0)], jnp.int32)
    other_rows = shift_rows[:, None] + global_rows[None]
    inside = (other_rows >= 0) & (other_rows < total_rows)
    active = jnp.where(inside[:, :, None], contact_mask, 0).reshape(-1)
    codes, wide_count = pair_codes(rows_dev, cols_dev)
    list_shape = jax.ShapeDtypeStruct((block_count * 9 + UNROLL,), jnp.int32)
    inner_list, outer_list, pair_count = pl.pallas_call(
        functools.partial(list_kernel, own=block_count),
        in_specs=[smem(), smem()],
        out_specs=(smem(), smem(), smem()),
        out_shape=(list_shape, list_shape, jax.ShapeDtypeStruct((2,), jnp.int32)),
        cost_estimate=pl.CostEstimate(flops=10**7, transcendentals=0, bytes_accessed=10**4),
        name="pairlist",
    )(active, jnp.asarray(codes))

    add_np, scale_np = shift_tables()
    add_tab = jnp.asarray(add_np, jnp.bfloat16)
    scale_tab = jnp.asarray(scale_np, jnp.bfloat16)

    ones = jnp.ones_like(radius)
    zeros = jnp.zeros_like(radius)
    length = disc_pos[0] * disc_pos[0] + disc_pos[1] * disc_pos[1] + 0.5 * SOFTEN
    state = jnp.stack([disc_pos[0], disc_pos[1], length, ones, radius, ones, zeros, zeros], axis=2)
    over_mass = 1.0 / ((radius / 0.06) ** 2)
    vel = jnp.stack([disc_vel[0], disc_vel[1], over_mass] + [zeros] * 5, axis=2)
    vel = vel.reshape(block_count, 8, disc_count)
    bonds = bond_list.reshape(BONDS, block_count, disc_count)
    near_scratch = [
        pltpu.VMEM((block_count + 1, 48, 4 * disc_count), jnp.bfloat16),
        pltpu.VMEM((block_count + 1, 32, 3 * disc_count), jnp.bfloat16),
    ]
    acc_shape = (block_count + 1, 16, disc_count)

    def substep(state, vel):
        state, left, right, low, high = halos(state)
        own = state.reshape(block_count, 8, disc_count)
        inner = pl.pallas_call(
            inner_kernel,
            in_specs=[smem(), smem()] + [vmem()] * 3,
            out_specs=vmem(),
            out_shape=jax.ShapeDtypeStruct(acc_shape, f32),
            scratch_shapes=[pltpu.VMEM((block_count, disc_count, DEPTH), jnp.bfloat16)]
            + near_scratch,
            cost_estimate=pl.CostEstimate(
                flops=8 * 10**9, transcendentals=10**7, bytes_accessed=2 * 10**6
            ),
            name="inner",
        )(pair_count, inner_list, own, add_tab, scale_tab)
        own, vel = pl.pallas_call(
            outer_kernel,
            in_specs=[smem(), smem()] + [vmem()] * 10,
            out_specs=(vmem(), vmem()),
            out_shape=(
                jax.ShapeDtypeStruct(own.shape, f32),
                jax.ShapeDtypeStruct(own.shape, f32),
            ),
            scratch_shapes=[
                pltpu.VMEM((wide_count - block_count + 1, disc_count, DEPTH), jnp.bfloat16)
            ]
            + near_scratch
            + [pltpu.VMEM(acc_shape, f32)],
            cost_estimate=pl.CostEstimate(
                flops=10**9, transcendentals=10**6, bytes_accessed=4 * 10**6
            ),
            name="outer",
        )(
            pair_count,
            outer_list,
            own,
            left,
            right,
            low,
            high,
            vel,
            bonds,
            add_tab,
            scale_tab,
            inner,
        )
        return own.reshape(rows_dev, cols_dev, 8, disc_count), vel

    state, vel = substep(state, vel)
    state, west, east, from_south, from_north, tops = lax.optimization_barrier(
        (state, west, east, from_south, from_north, tops)
    )

    is_top = (lax.axis_index("gy") == lat_tiles - 1).astype(jnp.int32).reshape(1)
    latitude = (lax.axis_index("gy") * tile_rows + jnp.arange(tile_rows, dtype=jnp.int32)).astype(
        f32
    )
    coriolis = SPIN_RATE * (2.0 * (latitude + 0.5) / (tile_rows * lat_tiles) - 1.0)
    coriolis = jnp.broadcast_to(coriolis[:, None], (tile_rows, tile_cols))
    chunk = next(size for size in (6, 4, 3, 2, 1) if layers % size == 0)

    def whole(shape):
        return pl.BlockSpec(shape, lambda g: (0,) * len(shape))

    def layer_block(size, index):
        return pl.BlockSpec(
            (fields, size, tile_rows, tile_cols), lambda g: (0, index(g), 0, 0)
        )

    updated = pl.pallas_call(
        ocean_kernel,
        grid=(layers // chunk,),
        in_specs=[
            smem(),
            layer_block(chunk, lambda g: g),
            layer_block(1, lambda g: jnp.maximum(g * chunk - 1, 0)),
            layer_block(1, lambda g: jnp.minimum(g * chunk + chunk, layers - 1)),
            pl.BlockSpec((chunk, tile_rows, tile_cols), lambda g: (g, 0, 0)),
            whole(west.shape),
            whole(east.shape),
            whole(from_south.shape),
            whole(from_north.shape),
            whole(tops.shape),
            whole((1, tile_cols)),
            whole(coriolis.shape),
        ],
        out_specs=layer_block(chunk, lambda g: g),
        out_shape=jax.ShapeDtypeStruct(ocean_state.shape, f32),
        scratch_shapes=[
            pltpu.VMEM((planes, tile_cols), f32),
            pltpu.VMEM((tile_cols, tile_cols), f32),
            pltpu.VMEM((tile_cols, tile_cols), f32),
        ],
        cost_estimate=pl.CostEstimate(flops=10**8, transcendentals=0, bytes_accessed=7 * 10**6),
        name="ocean",
    )(
        is_top,
        ocean_state,
        ocean_state,
        ocean_state,
        mix_coef,
        west,
        east,
        from_south,
        from_north,
        tops,
        fold_perm.reshape(1, tile_cols),
        coriolis,
    )

    cells = remap_cell[0].reshape(-1)
    surface = updated[0:2, 0].reshape(2, tile_rows * tile_cols)
    unforced = jnp.take(surface, cells, axis=1).reshape(2, tile_count, capacity)
    early = jnp.concatenate(
        [
            jnp.broadcast_to(cells.astype(f32)[None], (tile_count, slots)),
            unforced.transpose(1, 0, 2).reshape(tile_count, 2 * capacity),
        ],
        axis=1,
    )
    early = lax.all_to_all(early, ("gx", "gy"), split_axis=0, concat_axis=0, tiled=True)
    for step in range(1, SUB):
        state, vel = substep(state, vel)
        if step == 1:
            state, early = lax.optimization_barrier((state, early))
    all_cells = early[:, :slots].reshape(tile_count, tile_count, capacity)
    unforced = early[:, slots:].reshape(tile_count, 2, capacity)

    vel_rows = vel[:, 0:2]
    weight = radius.reshape(block_count, 1, disc_count) ** 2
    impulse = DRAG_ICE * jnp.sum(weight * vel_rows, axis=-1)
    selector = (
        remap_block[0].reshape(-1)[:, None] == jnp.arange(block_count, dtype=jnp.int32)[None]
    ).astype(f32)
    outgoing = lax.dot_general(
        impulse, selector, (((0,), (1,)), ((), ())), precision=HIGHEST
    ).reshape(1, 2 * slots)
    arrived = lax.all_to_all(
        jnp.broadcast_to(outgoing, (tile_count, 2 * slots)),
        ("gx", "gy"),
        split_axis=0,
        concat_axis=0,
        tiled=True,
    ).reshape(tile_count, 2, tile_count, capacity)

    tile_id = lax.axis_index("gx") * lat_tiles + lax.axis_index("gy")
    mine = lax.dynamic_index_in_dim(all_cells, tile_id, axis=1, keepdims=False)
    same = all_cells[:, None] == mine[:, :, None, None]
    landed = arrived.transpose(1, 2, 0, 3)
    forced = jnp.sum(jnp.where(same[None], landed[:, :, None], 0.0), axis=(3, 4))
    current = unforced.transpose(1, 0, 2) + forced
    per_block = jnp.dot(current.reshape(2, slots), selector, precision=HIGHEST)
    per_block = per_block.reshape(2, rows_dev, cols_dev)
    velocity = vel.reshape(rows_dev, cols_dev, 8, disc_count)[:, :, 0:2].transpose(2, 0, 1, 3)
    position = state[:, :, 0:2].transpose(2, 0, 1, 3)
    vel_next = velocity + DRAG_BACK * (per_block[..., None] - velocity)

    here = lax.dynamic_index_in_dim(arrived, tile_id, axis=2, keepdims=False)
    here = here.transpose(1, 0, 2).reshape(2, 1, slots)
    in_row = (cells // tile_cols)[None] == jnp.arange(tile_rows, dtype=jnp.int32)[:, None]
    in_col = (cells % tile_cols)[:, None] == jnp.arange(tile_cols, dtype=jnp.int32)[None]
    forcing = jnp.dot(
        jnp.where(in_row[None], here, 0.0).reshape(2 * tile_rows, slots),
        in_col.astype(f32),
        precision=HIGHEST,
    ).reshape(2, tile_rows, tile_cols)
    updated = updated.at[0:2, 0].add(forcing)
    return (position, vel_next, updated)


def solution(mesh):
    in_specs = (
        P(None, "gy", "gx", None),
        P(None, "gy", "gx", None),
        P("gy", "gx", None),
        P(None, "gy", "gx", None),
        P(None, "gy", "gx"),
        P(("gx", "gy"), None, None),
        P(None, None, "gy", "gx"),
        P(None, "gy", "gx"),
        P(("gx", "gy"), None, None),
        P("gx"),
    )
    out_specs = (P(None, "gy", "gx", None), P(None, "gy", "gx", None), P(None, None, "gy", "gx"))
    return jax.shard_map(body, mesh=mesh, in_specs=in_specs, out_specs=out_specs, check_vma=False)
```
